32 devices in a mesh: row: 4 (over z), col: 8 (over y, x, core).
Axes of the slice: x: 2, y: 2, z: 4, core: 2. Of those that a mesh axis runs over, the one named last changes fastest.
Arguments:
- green: float32 [512, 16384], P(('row', 'col')), may hold values from -0.375 to 0.375
- noise_precision: float32 [512], P(('row', 'col')), may hold values from 0.5 to 4
- data_set: int32 [512], P(('row', 'col')), may hold values from 0 to 3
- set_scale: float32 [4], replicated, may hold values from 0.5 to 2
- stiffness: float32 [8192], replicated, may hold values from 0.25 to 2
- patch_cell: int32 [8192], replicated, may hold values from 0 to 8191, each once
Outputs:
- precision_matrix: float32 [16384, 16384], P('row', 'col')
The draws below stay inside these ranges and needn't reach their ends.
Inputs may be any that keep to these rules, and one draw needn't show every extreme that they name: `patch_cell`: every cell 0 to 8191 holds exactly one patch.
All inputs are finite; a program needn't handle non-finite values.
Results may differ from the reference program's by a relative error of at most 0.00005.
Values sent between devices are 32-bit elements; how exact they have to be, the bound alone decides.
A program may use at most 256 MiB of HBM per device.

```python
import math
import jax
import jax.numpy as jnp
from jax import lax

NSTRIKE = 128
NDIP = 64
NSETS = 4
O = 512
P_SIZE = 8192
M = 16384


def place_ends(entries, stream_key, least, high):
    shape = entries.shape
    place = [jax.random.randint(jax.random.fold_in(stream_key, axis), (), 0, shape[axis]) for axis in range(len(shape))]
    entries = entries.at[tuple(place)].set(least)
    longest = shape.index(max(shape))
    place[longest] = (place[longest] + 1) % shape[longest]
    return entries.at[tuple(place)].set(high)


def levels(rng, shape, cuts, low, largest):
    def one(position, blocks):
        draws = jax.random.uniform(jax.random.fold_in(jax.random.fold_in(rng, 6), position), (blocks,), jnp.float32, low / len(cuts), largest / len(cuts))
        return jnp.repeat(jnp.exp(draws), shape[position] // blocks).reshape((-1,) + (1,) * (len(shape) - position - 1))

    level = one(*cuts[0])
    for cut in cuts[1:]:
        level = level * one(*cut)
    return level


def gaussian(key, extent, scale, bound, cuts=(), kind=jnp.bfloat16):
    result = scale * jax.random.normal(key, extent, jnp.float32)
    if cuts:
        result = result * levels(key, extent, cuts, -0.22, 0.18)
    return jnp.clip(result, -bound, bound).astype(kind)


def setup_inputs(seed: int = 0) -> dict:
    splits = jax.random.split(jax.random.key(seed), 7)
    return {
        "green": gaussian(splits[0], (O, M), (O // 2) ** -0.5, 0.375, ((0, 32),), jnp.float32),
        "noise_precision": jnp.clip(jnp.exp(math.log(4.0) - 2.0794415 * jax.random.uniform(splits[1], (O,), jnp.float32) ** levels(splits[1], (O,), ((0, 32),), -0.2, 0.2)), 0.5, 4.0),
        "data_set": place_ends(jax.random.randint(splits[2], (O,), 0, NSETS), jax.random.fold_in(splits[2], 1), 0, NSETS - 1).astype(jnp.int32),
        "set_scale": jnp.clip(jnp.exp(jax.random.uniform(splits[3], (NSETS,), jnp.float32, math.log(0.5), math.log(2.0))), 0.5, 2.0),
        "stiffness": jnp.clip(jnp.exp(jax.random.uniform(splits[4], (P_SIZE,), jnp.float32, math.log(0.25), math.log(2.0))), 0.25, 2.0),
        "patch_cell": jax.random.permutation(splits[5], P_SIZE).astype(jnp.int32),
    }


def reference(green, noise_precision, data_set, set_scale, stiffness, patch_cell):
    weight = noise_precision * set_scale[data_set]
    scaled = green * jnp.sqrt(weight)[:, None]
    precision_matrix = lax.dot_general(scaled, scaled, (((0,), (0,)), ((), ())), precision=lax.Precision.HIGHEST, preferred_element_type=jnp.float32)
    patch_count = NSTRIKE * NDIP
    cell_ids = jnp.arange(patch_count, dtype=jnp.int32)
    owner = jnp.zeros((patch_count,), jnp.int32).at[patch_cell].set(cell_ids)
    strike_pos = cell_ids // NDIP
    dip_pos = cell_ids % NDIP
    along = owner[jnp.minimum(cell_ids + NDIP, patch_count - 1)]
    below = owner[jnp.minimum(cell_ids + 1, patch_count - 1)]
    heads = jnp.concatenate([owner, owner])
    tails = jnp.concatenate([along, below])
    valid = jnp.concatenate([strike_pos < NSTRIKE - 1, dip_pos < NDIP - 1])
    edges = jnp.where(valid, 0.5 * (stiffness[heads] + stiffness[tails]), 0.0)
    row_list = []
    col_list = []
    values = []
    for component in range(2):
        first_ids = (component * patch_count + heads).astype(jnp.int32)
        second_ids = (component * patch_count + tails).astype(jnp.int32)
        row_list += [first_ids, second_ids, first_ids, second_ids]
        col_list += [second_ids, first_ids, first_ids, second_ids]
        values += [-edges, -edges, edges, edges]
    return precision_matrix.at[jnp.concatenate(row_list), jnp.concatenate(col_list)].add(jnp.concatenate(values))
```

```python
import jax
import jax.numpy as jnp
from jax import lax
from jax.experimental import pallas as pl
from jax.experimental.pallas import tpu as pltpu
from jax.sharding import PartitionSpec as P

NSTRIKE = 128
NDIP = 64


def gram_product(left_panel, right_panel):
    return lax.dot_general(
        left_panel,
        right_panel,
        (((0,), (0,)), ((), ())),
        precision=lax.Precision.HIGH,
        preferred_element_type=jnp.float32,
    )


def one_hots(cells):
    strike_hot = cells[:, None] // NDIP == jnp.arange(NSTRIKE, dtype=jnp.int32)[None, :]
    dip_hot = cells[:, None] % NDIP == jnp.arange(NDIP, dtype=jnp.int32)[None, :]
    return strike_hot, dip_hot


def degree_table(stiffness, patch_cell):
    strike_hot, dip_hot = one_hots(patch_cell)
    grid = lax.dot_general(
        strike_hot.astype(jnp.float32),
        jnp.where(dip_hot, stiffness[:, None], 0.0),
        (((0,), (0,)), ((), ())),
        precision=lax.Precision.HIGHEST,
        preferred_element_type=jnp.float32,
    )
    padded = jnp.pad(grid, 1)
    strike_ids = lax.broadcasted_iota(jnp.int32, (NSTRIKE, NDIP), 0)
    dip_ids = lax.broadcasted_iota(jnp.int32, (NSTRIKE, NDIP), 1)
    degree = jnp.zeros((NSTRIKE, NDIP), jnp.float32)
    degree = degree + jnp.where(strike_ids < NSTRIKE - 1, 0.5 * (grid + padded[2:, 1:-1]), 0.0)
    degree = degree + jnp.where(strike_ids > 0, 0.5 * (grid + padded[:-2, 1:-1]), 0.0)
    degree = degree + jnp.where(dip_ids < NDIP - 1, 0.5 * (grid + padded[1:-1, 2:]), 0.0)
    degree = degree + jnp.where(dip_ids > 0, 0.5 * (grid + padded[1:-1, :-2]), 0.0)
    return degree


def degree_of(degree, cells):
    strike_hot, dip_hot = one_hots(cells)
    lines = jnp.dot(
        strike_hot.astype(jnp.float32),
        degree,
        precision=lax.Precision.HIGHEST,
        preferred_element_type=jnp.float32,
    )
    return jnp.sum(jnp.where(dip_hot, lines, 0.0), axis=1)


def smoothing_tile(stiffness, patch_cell, row_start, tile_height, col_start, tile_width):
    patch_count = stiffness.shape[0]
    degree_cells = degree_table(stiffness, patch_cell)
    row_first = row_start % patch_count
    col_first = col_start % patch_count
    row_cell = lax.dynamic_slice_in_dim(patch_cell, row_first, tile_height, 0)
    col_cell = lax.dynamic_slice_in_dim(patch_cell, col_first, tile_width, 0)
    row_stiff = lax.dynamic_slice_in_dim(stiffness, row_first, tile_height, 0)
    col_stiff = lax.dynamic_slice_in_dim(stiffness, col_first, tile_width, 0)
    row_degree = degree_of(degree_cells, row_cell)
    row_strike = row_cell // NDIP
    row_dip = row_cell % NDIP
    col_strike = col_cell // NDIP
    col_dip = col_cell % NDIP
    spacing = jnp.abs(row_strike[:, None] - col_strike[None, :]) + jnp.abs(
        row_dip[:, None] - col_dip[None, :]
    )
    row_ids = row_start + jnp.arange(tile_height, dtype=jnp.int32)
    col_ids = col_start + jnp.arange(tile_width, dtype=jnp.int32)
    same_part = row_ids[:, None] // patch_count == col_ids[None, :] // patch_count
    coupling = jnp.where(
        (spacing == 1) & same_part, -0.5 * (row_stiff[:, None] + col_stiff[None, :]), 0.0
    )
    diagonal = row_ids[:, None] == col_ids[None, :]
    return coupling + jnp.where(diagonal, row_degree[:, None], 0.0)


def exchange_kernel(row_count, col_count, block, by_row, by_column, send, recv, own):
    row = lax.axis_index("row")
    col = lax.axis_index("col")
    rows = block.shape[0]
    height = by_row.shape[1]
    width = by_column.shape[1]
    row_slot = by_row.at[pl.ds(pl.multiple_of(row * rows, 8), rows), :]
    col_slot = by_column.at[pl.ds(pl.multiple_of(col * rows, 8), rows), :]
    copies = []
    for step in range(1, row_count):
        target = lax.rem(row + step, row_count)
        copies.append(
            pltpu.make_async_remote_copy(
                src_ref=block.at[:, pl.ds(pl.multiple_of(target * height, 128), height)],
                dst_ref=row_slot,
                send_sem=send.at[step - 1],
                recv_sem=recv.at[step - 1],
                device_id=(target, col),
                device_id_type=pl.DeviceIdType.MESH,
            )
        )
    for step in range(1, col_count):
        target = lax.rem(col + step, col_count)
        copies.append(
            pltpu.make_async_remote_copy(
                src_ref=block.at[:, pl.ds(pl.multiple_of(target * width, 128), width)],
                dst_ref=col_slot,
                send_sem=send.at[row_count + step - 2],
                recv_sem=recv.at[row_count + step - 2],
                device_id=(row, target),
                device_id_type=pl.DeviceIdType.MESH,
            )
        )
    copies.append(
        pltpu.make_async_copy(
            block.at[:, pl.ds(pl.multiple_of(row * height, 128), height)], row_slot, own.at[0]
        )
    )
    copies.append(
        pltpu.make_async_copy(
            block.at[:, pl.ds(pl.multiple_of(col * width, 128), width)], col_slot, own.at[1]
        )
    )
    for copy in copies:
        copy.start()
    for copy in copies:
        copy.wait()


def exchange(scaled, row_count, col_count):
    rows, order_full = scaled.shape
    in_vmem = pl.BlockSpec(memory_space=pltpu.VMEM)
    partners = row_count + col_count - 2

    def body(*refs):
        exchange_kernel(row_count, col_count, *refs)

    return pl.pallas_call(
        body,
        out_shape=(
            jax.ShapeDtypeStruct((row_count * rows, order_full // row_count), jnp.float32),
            jax.ShapeDtypeStruct((col_count * rows, order_full // col_count), jnp.float32),
        ),
        in_specs=[in_vmem],
        out_specs=(in_vmem, in_vmem),
        scratch_shapes=[
            pltpu.SemaphoreType.DMA((partners,)),
            pltpu.SemaphoreType.DMA((partners,)),
            pltpu.SemaphoreType.DMA((2,)),
        ],
        compiler_params=pltpu.CompilerParams(has_side_effects=True),
    )(scaled)


def per_device(green, noise_precision, data_set, set_scale, stiffness, patch_cell):
    row_count = lax.axis_size("row")
    col_count = lax.axis_size("col")
    local_rows = green.shape[0]
    order_full = green.shape[1]
    tile_height = order_full // row_count
    tile_width = order_full // col_count
    matches = data_set[:, None] == jnp.arange(set_scale.shape[0], dtype=jnp.int32)[None, :]
    weight = noise_precision * jnp.sum(jnp.where(matches, set_scale[None, :], 0.0), axis=1)
    scaled = green * jnp.sqrt(weight)[:, None]
    by_row, by_column = exchange(scaled, row_count, col_count)
    right_factor = lax.all_gather(by_column, "row", axis=0, tiled=True)
    reordered = jnp.transpose(
        right_factor.reshape(row_count, col_count, local_rows, tile_width), (1, 0, 2, 3)
    ).reshape(row_count * col_count * local_rows, tile_width)
    gram_tile = gram_product(lax.all_gather(by_row, "col", axis=0, tiled=True), reordered)
    prior = smoothing_tile(
        stiffness,
        patch_cell,
        lax.axis_index("row") * tile_height,
        tile_height,
        lax.axis_index("col") * tile_width,
        tile_width,
    )
    return gram_tile + prior


def solution(mesh):
    placed = (P(("row", "col"), None), P(("row", "col")), P(("row", "col")), P(), P(), P())
    return jax.shard_map(
        per_device, mesh=mesh, in_specs=placed, out_specs=P("row", "col"), check_vma=False
    )
```
